512 devices in a mesh: cells: 64 (over x, y, z_lo), src: 8 (over z_hi, core).
Axes of the slice: x: 4, y: 8, z: 8 (z_hi: 4, z_lo: 2; z = z_hi * 2 + z_lo), core: 2. Of those that a mesh axis runs over, the one named last changes fastest.
Arguments:
- conductivity: float32 [256, 1024], P('cells'), may hold values from 0.2 to 5
- prev_fields: bfloat16 [1024, 256, 1024], P('src', 'cells'), may hold values from -6 to 6
- electrodes: int32 [1024, 2], P('src'), may hold values from 0 to 262143, as said below
- data_weight: bfloat16 [1024, 1024], replicated, may hold values from -3 to 4
Outputs:
- potentials: bfloat16 [1024, 256, 1024], P('src', 'cells')
- gradient: float32 [256, 1024], P('cells', 'src')
The draws below stay inside these ranges and needn't reach their ends.
Inputs may be any that keep to these rules, and one draw needn't show every extreme that they name: `electrodes`: in each row the two cells differ.
All inputs are finite; a program needn't handle non-finite values.
Results may differ from the reference program's by a relative error of at most 0.0034.
Values may be sent and summed in bfloat16 or wider, within the bound.
A program may use at most 64 MiB of HBM per device.

```python
import math
import jax
import jax.numpy as jnp
from jax import lax

S = 1024
NX = 32
NY = 32
ITERS = 2
NZ = 256


def draw_electrodes(key, part):
    first_key, second_key = jax.random.split(jax.random.fold_in(key, 5))
    ncell = NZ * NX * NY
    source_cell = jax.random.randint(first_key, (S,), 0, ncell, dtype=jnp.int32)
    stride = jax.random.randint(second_key, (S,), 1, ncell, dtype=jnp.int32)
    sink_cell = (source_cell + stride) % ncell
    return jnp.stack([source_cell, sink_cell], axis=1).astype(jnp.int32)


def draw_data_weight(key, part):
    first_key, second_key = jax.random.split(jax.random.fold_in(key, 11))
    scales = jnp.exp(jax.random.uniform(first_key, (S,), jnp.float32, math.log(0.1), 0.0))
    spread = jnp.clip(jax.random.normal(second_key, (S, S), jnp.float32), -4.0, 4.0)
    weights = jnp.diag(scales) + spread * (4.0 / math.sqrt(S))
    return weights.astype(jnp.bfloat16)


def level_of(own_key, dims, shards, low, high):
    def one(dim, shards_of):
        steps = jax.random.uniform(jax.random.fold_in(jax.random.fold_in(own_key, 6), dim), (shards_of,), jnp.float32, low / len(shards), high / len(shards))
        return jnp.repeat(jnp.exp(steps), dims[dim] // shards_of).reshape((-1,) + (1,) * (len(dims) - dim - 1))

    factor_of = one(*shards[0])
    for cut in shards[1:]:
        factor_of = factor_of * one(*cut)
    return factor_of


def gaussian(own_key, shape, scale, bound, cuts=(), kind=jnp.bfloat16):
    drawn = scale * jax.random.normal(own_key, shape, jnp.float32)
    if cuts:
        drawn = drawn * level_of(own_key, shape, cuts, -0.22, 0.18)
    return jnp.clip(drawn, -bound, bound).astype(kind)


def setup_inputs(seed: int = 0) -> dict:
    key_list = jax.random.split(jax.random.key(seed), 5)
    conductivity = jnp.clip(jnp.exp(math.log(5.0) - 3.218876 * jax.random.uniform(key_list[0], (NZ, NX * NY), jnp.float32) ** level_of(key_list[0], (NZ, NX * NY), ((0, 64),), -0.2, 0.2)), 0.2, 5.0)
    prev_fields = gaussian(key_list[1], (S, NZ, NX * NY), 1.0, 6.0, ((0, 8), (1, 64)))
    electrodes = draw_electrodes(jax.random.fold_in(key_list[4], 71), 0)
    data_weight = draw_data_weight(jax.random.fold_in(key_list[4], 71), 0)
    return {"conductivity": conductivity, "prev_fields": prev_fields, "electrodes": electrodes, "data_weight": data_weight}


relaxation = 2.0 / 3.0
current = 4.0


def shift_last(values, offset):
    if offset > 0:
        padding = jnp.zeros(values.shape[:-1] + (offset,), values.dtype)
        return jnp.concatenate([values[..., offset:], padding], axis=-1)
    padding = jnp.zeros(values.shape[:-1] + (-offset,), values.dtype)
    return jnp.concatenate([padding, values[..., :offset]], axis=-1)


def column_masks(length, row_len):
    column = jnp.arange(length, dtype=jnp.int32) % row_len
    return (column != row_len - 1).astype(jnp.float32), (column != 0).astype(jnp.float32)


def coefficients(sigma_pad, row_len):
    sigma = sigma_pad[1:-1]
    upper_mask, lower_mask = column_masks(sigma.shape[-1], row_len)
    z_plus = 0.5 * (sigma + sigma_pad[2:])
    z_minus = 0.5 * (sigma + sigma_pad[:-2])
    y_plus = 0.5 * (sigma + shift_last(sigma, 1) * upper_mask)
    y_minus = 0.5 * (sigma + shift_last(sigma, -1) * lower_mask)
    x_plus = 0.5 * (sigma + shift_last(sigma, row_len))
    x_minus = 0.5 * (sigma + shift_last(sigma, -row_len))
    diagonal = z_plus + z_minus + y_plus + y_minus + x_plus + x_minus
    return (z_plus, z_minus, y_plus, y_minus, x_plus, x_minus, diagonal, upper_mask, lower_mask)


def relax(fields_pad, source, coeffs, row_len):
    z_plus, z_minus, y_plus, y_minus, x_plus, x_minus, diagonal, upper_mask, lower_mask = coeffs
    fields = fields_pad[:, 1:-1]
    applied = diagonal * fields - z_plus * fields_pad[:, 2:] - z_minus * fields_pad[:, :-2]
    applied = applied - y_plus * (shift_last(fields, 1) * upper_mask) - y_minus * (shift_last(fields, -1) * lower_mask)
    applied = applied - x_plus * shift_last(fields, row_len) - x_minus * shift_last(fields, -row_len)
    return fields + relaxation * (source - applied) / diagonal


def differences(planes, above, beside, row_len):
    upper_mask, lower_mask = column_masks(planes.shape[-1], row_len)
    along_x = jnp.concatenate([planes[..., row_len:], beside], axis=-1)
    along_y = shift_last(planes, 1) * upper_mask
    along_z = jnp.concatenate([planes[:, 1:], above], axis=1)
    return tuple((shifted - planes).astype(jnp.bfloat16) for shifted in (along_x, along_y, along_z))


def weigh(diffs, data_weight):
    count = data_weight.shape[0]
    total = jnp.zeros(diffs[0].shape[1:], jnp.float32)
    for block in diffs:
        flat = block.reshape(count, -1)
        mixed = jnp.dot(data_weight, flat, preferred_element_type=jnp.float32)
        total = total + jnp.sum(flat.astype(jnp.float32) * mixed, axis=0).reshape(total.shape)
    return total / count


def reference(conductivity, prev_fields, electrodes, data_weight):
    ncell = NZ * NX * NY
    sigma_pad = jnp.pad(conductivity, ((1, 1), (0, 0)))
    coeffs = coefficients(sigma_pad, NY)
    width = min(128, S)
    cell_ids = jnp.arange(ncell, dtype=jnp.int32)

    def solve_block(inputs):
        start_fields, pairs = inputs
        source = current * ((cell_ids[None, :] == pairs[:, 0:1]).astype(jnp.float32)
                            - (cell_ids[None, :] == pairs[:, 1:2]).astype(jnp.float32))
        source = source.reshape(width, NZ, NX * NY)
        fields = start_fields.astype(jnp.float32)
        for sweep in range(ITERS):
            fields_pad = jnp.pad(fields, ((0, 0), (1, 1), (0, 0)))
            fields = relax(fields_pad, source, coeffs, NY)
        return fields.astype(jnp.bfloat16)

    blocks = lax.map(solve_block, (prev_fields.reshape(S // width, width, NZ, NX * NY),
                                   electrodes.reshape(S // width, width, 2)))
    potentials = blocks.reshape(S, NZ, NX * NY)
    padded = jnp.pad(potentials, ((0, 0), (0, 1), (0, 0)))

    def plane_gradient(level):
        slab = lax.dynamic_slice_in_dim(padded, level, 2, 1).astype(jnp.float32)
        beside = jnp.zeros((S, 1, NY), jnp.float32)
        return weigh(differences(slab[:, :1], slab[:, 1:], beside, NY), data_weight)

    gradient = lax.map(plane_gradient, jnp.arange(NZ, dtype=jnp.int32)).reshape(NZ, NX * NY)
    return potentials, gradient
```

```python
import jax
import jax.numpy as jnp
from jax import lax
from jax.experimental import pallas as pl
from jax.experimental.pallas import tpu as pltpu
from jax.sharding import PartitionSpec as P

NY = 32
LANES = 128
CHUNKS = 4
GROUP = 16
relaxation = 2.0 / 3.0
current = 4.0
MESH = pl.DeviceIdType.MESH


def kernel(
    cond, prev, electrodes, weight_hbm, pot, grad,
    halo, sigma_halo, coef, first, packed, gathered, partner, above, beside, weight, diffs,
    halo_send, halo_recv, sigma_send, sigma_recv, main_send, main_recv, side_send, side_recv,
    above_send, above_recv, partner_send, partner_recv, weight_sem,
):
    slabs, groups = lax.axis_size("cells"), lax.axis_size("src")
    depth, local, plane = prev.shape
    tiles = plane // LANES
    rows = local // CHUNKS
    count = groups * local
    k, j = lax.axis_index("cells"), lax.axis_index("src")
    odd = lax.rem(j, 2) == 1
    has_low, has_high = k > 0, k < slabs - 1
    sided = jnp.logical_and(odd, j < groups - 1)

    weight_copy = pltpu.make_async_copy(weight_hbm, weight, weight_sem)
    weight_copy.start()

    barrier = pltpu.get_barrier_semaphore()

    @pl.when(has_low)
    def _():
        pl.semaphore_signal(barrier, inc=1, device_id=(k - 1, j), device_id_type=MESH)

    @pl.when(has_high)
    def _():
        pl.semaphore_signal(barrier, inc=1, device_id=(k + 1, j), device_id_type=MESH)

    for r in range(1, groups):
        pl.semaphore_signal(
            barrier, inc=1, device_id=(k, lax.rem(j + r, groups)), device_id_type=MESH
        )
    pl.semaphore_wait(
        barrier, groups - 1 + has_low.astype(jnp.int32) + has_high.astype(jnp.int32)
    )

    def sigma_copy(side):
        return pltpu.make_async_remote_copy(
            src_ref=cond.at[pl.ds(2 - 2 * side, 2)],
            dst_ref=sigma_halo.at[side],
            send_sem=sigma_send.at[side],
            recv_sem=sigma_recv.at[side],
            device_id=(k + 1 - 2 * side, j),
            device_id_type=MESH,
        )

    def halo_copy(side, chunk):
        span = pl.ds(pl.multiple_of(chunk * rows, rows), rows)
        return pltpu.make_async_remote_copy(
            src_ref=prev.at[pl.ds(2 - 2 * side, 2), span],
            dst_ref=halo.at[side, :, span],
            send_sem=halo_send.at[side, chunk],
            recv_sem=halo_recv.at[side, chunk],
            device_id=(k + 1 - 2 * side, j),
            device_id_type=MESH,
        )

    def main_copy(r, chunk):
        peer = lax.rem(j + r, groups)
        span = pl.ds(pl.multiple_of(chunk * rows, rows), rows)
        band = pl.ds(pl.multiple_of(peer * LANES, LANES), LANES)
        return pltpu.make_async_remote_copy(
            src_ref=pot.at[:, span, band],
            dst_ref=gathered.at[:, j, span],
            send_sem=main_send.at[r - 1, chunk],
            recv_sem=main_recv.at[r - 1, chunk],
            device_id=(k, peer),
            device_id_type=MESH,
        )

    def side_copy(r, chunk):
        peer = lax.rem(j + r, groups)
        span = pl.ds(pl.multiple_of(chunk * rows, rows), rows)
        return pltpu.make_async_remote_copy(
            src_ref=packed.at[lax.rem(peer + 1, groups), span],
            dst_ref=beside.at[j, span],
            send_sem=side_send.at[r - 1, chunk],
            recv_sem=side_recv.at[r - 1, chunk],
            device_id=(k, peer),
            device_id_type=MESH,
        )

    def takes_side(peer):
        return jnp.logical_and(lax.rem(peer, 2) == 1, peer < groups - 1)

    def above_copy(chunk):
        span = pl.ds(pl.multiple_of(chunk * rows, rows), rows)
        return pltpu.make_async_remote_copy(
            src_ref=gathered.at[0, :, span],
            dst_ref=above.at[:, span],
            send_sem=above_send.at[chunk],
            recv_sem=above_recv.at[chunk],
            device_id=(k - 1, j),
            device_id_type=MESH,
        )

    def partner_copy(chunk):
        span = pl.ds(pl.multiple_of(chunk * rows, rows), rows)
        return pltpu.make_async_remote_copy(
            src_ref=gathered.at[:, :, span],
            dst_ref=partner.at[:, :, span],
            send_sem=partner_send.at[chunk],
            recv_sem=partner_recv.at[chunk],
            device_id=(k, lax.rem(j - 1 + groups, groups)),
            device_id_type=MESH,
        )

    sends = ((has_high, 0), (has_low, 1))
    for present, side in sends:

        @pl.when(present)
        def _(side=side):
            sigma_copy(side).start()

    for chunk in range(CHUNKS):
        for present, side in sends:

            @pl.when(present)
            def _(side=side, chunk=chunk):
                halo_copy(side, chunk).start()

    receives = ((has_low, 0), (has_high, 1))
    for present, side in receives:

        @pl.when(jnp.logical_not(present))
        def _(side=side):
            sigma_halo[side] = jnp.zeros(sigma_halo.shape[1:], sigma_halo.dtype)
            halo[side] = jnp.zeros(halo.shape[1:], halo.dtype)

        @pl.when(present)
        def _(side=side):
            sigma_copy(side).wait_recv()

    @pl.when(jnp.logical_not(has_high))
    def _():
        above[...] = jnp.zeros(above.shape, above.dtype)

    @pl.when(j == groups - 1)
    def _():
        beside[...] = jnp.zeros(beside.shape, beside.dtype)

    cell = lax.broadcasted_iota(jnp.int32, (1, plane), 1)
    column = lax.rem(cell, NY)
    own = cond[...]
    low, high = sigma_halo[0], sigma_halo[1]
    sigma = (
        [low[i : i + 1] for i in range(2)]
        + [own[i : i + 1] for i in range(depth)]
        + [high[i : i + 1] for i in range(2)]
    )
    for p in range(depth + 2):
        s, down, up = sigma[p + 1], sigma[p], sigma[p + 2]
        y_up = jnp.where(column != NY - 1, pltpu.roll(s, plane - 1, 1), 0.0)
        y_down = jnp.where(column != 0, pltpu.roll(s, 1, 1), 0.0)
        x_up = jnp.where(cell < plane - NY, pltpu.roll(s, plane - NY, 1), 0.0)
        x_down = jnp.where(cell >= NY, pltpu.roll(s, NY, 1), 0.0)
        faces = [0.5 * (s + o) for o in (up, down, y_up, y_down, x_up, x_down)]
        diagonal = faces[0] + faces[1] + faces[2] + faces[3] + faces[4] + faces[5]
        scale = relaxation / diagonal
        center = jnp.full((1, plane), 1.0 - relaxation, jnp.float32)
        if p == 0:
            scale = jnp.where(has_low, scale, 0.0)
            center = jnp.where(has_low, center, 0.0)
        if p == depth + 1:
            scale = jnp.where(has_high, scale, 0.0)
            center = jnp.where(has_high, center, 0.0)
        terms = [
            faces[0] * scale,
            faces[1] * scale,
            jnp.where(column != NY - 1, faces[2] * scale, 0.0),
            jnp.where(column != 0, faces[3] * scale, 0.0),
            jnp.where(cell < plane - NY, faces[4] * scale, 0.0),
            jnp.where(cell >= NY, faces[5] * scale, 0.0),
            center,
            current * scale,
        ]
        for i, term in enumerate(terms):
            coef[p, i : i + 1, :] = term

    lane = lax.broadcasted_iota(jnp.int32, (GROUP, LANES), 1)
    first_cell = k * (depth * plane)

    def sweep(value, p, pair, store):
        low_cell = first_cell + (p - 1) * plane
        plus, minus = pair[0] - low_cell, pair[1] - low_cell
        mids = [value(p, v) for v in range(tiles)]
        ups = [pltpu.roll(m, LANES - NY, 1) for m in mids]
        downs = [pltpu.roll(m, NY, 1) for m in mids]
        for v in range(tiles):
            c = [coef[p, i : i + 1, v * LANES : (v + 1) * LANES] for i in range(8)]
            x_up = jnp.where(lane < LANES - NY, ups[v], ups[v + 1]) if v < tiles - 1 else ups[v]
            x_down = jnp.where(lane >= NY, downs[v], downs[v - 1]) if v > 0 else downs[v]
            total = c[6] * mids[v] + c[0] * value(p + 1, v) + c[1] * value(p - 1, v)
            total = total + c[2] * pltpu.roll(mids[v], LANES - 1, 1)
            total = total + c[3] * pltpu.roll(mids[v], 1, 1)
            total = total + c[4] * x_up + c[5] * x_down
            here = lane + v * LANES
            gain = jnp.broadcast_to(c[7], (GROUP, LANES))
            total = total + jnp.where(here == plus, gain, jnp.where(here == minus, -gain, 0.0))
            store(v, total)

    def relax_group(g):
        span = pl.ds(pl.multiple_of(g * GROUP, GROUP), GROUP)
        pair = electrodes[span, :]
        pair = [
            jnp.broadcast_to(pair[:, 0:1], (GROUP, LANES)),
            jnp.broadcast_to(pair[:, 1:2], (GROUP, LANES)),
        ]

        def start(q, v):
            at = slice(v * LANES, (v + 1) * LANES)
            if q < 1:
                block = halo[0, q + 1, span, at]
            elif q <= depth:
                block = prev[q - 1, span, at]
            else:
                block = halo[1, q - depth - 1, span, at]
            return block.astype(jnp.float32)

        for p in range(depth + 2):

            def keep(v, total, p=p):
                first[p, :, v * LANES : (v + 1) * LANES] = total

            sweep(start, p, pair, keep)

        heads = [[None] * depth for _ in range(tiles)]

        def middle(q, v):
            return first[q, :, v * LANES : (v + 1) * LANES]

        for p in range(1, depth + 1):

            def keep(v, total, p=p):
                pot[p - 1, span, v * LANES : (v + 1) * LANES] = total.astype(pot.dtype)
                if v % 2 == 0:
                    turned = total if p == 1 else pltpu.roll(total, (p - 1) * NY, 1)
                    if p == 1:
                        heads[v] = turned
                    else:
                        heads[v] = jnp.where(lane < (p - 1) * NY, heads[v], turned)

            sweep(middle, p, pair, keep)
        for v in range(0, tiles, 2):
            packed[v, span] = heads[v].astype(packed.dtype)

    per_chunk = rows // GROUP

    def relax_chunk(chunk, carry):
        for present, side in receives:

            @pl.when(present)
            def _(side=side):
                halo_copy(side, chunk).wait_recv()

        def one(g, carry):
            relax_group(chunk * per_chunk + g)
            return carry

        lax.fori_loop(0, per_chunk, one, 0)
        span = pl.ds(pl.multiple_of(chunk * rows, rows), rows)
        band = pl.ds(pl.multiple_of(j * LANES, LANES), LANES)
        for p in range(depth):
            gathered[p, j, span] = pot[p, span, band]

        @pl.when(sided)
        def _():
            beside[j, span] = packed[lax.rem(j + 1, groups), span]

        for r in range(1, groups):
            main_copy(r, chunk).start()

            @pl.when(takes_side(lax.rem(j + r, groups)))
            def _(r=r):
                side_copy(r, chunk).start()

        return carry

    lax.fori_loop(0, CHUNKS, relax_chunk, 0)

    def forward_chunk(chunk, carry):
        for r in range(1, groups):
            main_copy(r, chunk).wait_recv()

            @pl.when(sided)
            def _(r=r):
                side_copy(r, chunk).wait_recv()

        @pl.when(has_low)
        def _():
            above_copy(chunk).start()

        @pl.when(odd)
        def _():
            partner_copy(chunk).start()

        return carry

    lax.fori_loop(0, CHUNKS, forward_chunk, 0)

    block = 64
    per_group = local // block
    lane = lax.broadcasted_iota(jnp.int32, (block, LANES), 1)
    inner = lax.rem(lane, NY) != NY - 1

    def each_block(step):
        def one(i, carry):
            source = i // per_group
            span = pl.ds(pl.multiple_of(lax.rem(i, per_group) * block, block), block)
            step(source, span, pl.ds(pl.multiple_of(i * block, block), block))
            return carry

        lax.fori_loop(0, groups * per_group, one, 0)

    def put(d, p, at, value):
        diffs[d, at, p * LANES : (p + 1) * LANES] = value.astype(diffs.dtype)

    def along_y(source, span, at):
        for p in range(depth):
            here = gathered[p, source, span].astype(jnp.float32)
            put(1, p, at, jnp.where(inner, pltpu.roll(here, LANES - 1, 1), 0.0) - here)

    def along_x_odd(source, span, at):
        tail = beside[source, span].astype(jnp.float32)
        for p in range(depth):
            here = gathered[p, source, span].astype(jnp.float32)
            shift = (LANES - NY - NY * p) % LANES
            edge = pltpu.roll(tail, shift, 1) if shift else tail
            turned = pltpu.roll(here, LANES - NY, 1)
            put(0, p, at, jnp.where(lane < LANES - NY, turned, edge) - here)

    def along_x_even(source, span, at):
        for p in range(depth):
            here = gathered[p, source, span].astype(jnp.float32)
            edge = pltpu.roll(partner[p, source, span].astype(jnp.float32), LANES - NY, 1)
            turned = pltpu.roll(here, LANES - NY, 1)
            put(0, p, at, jnp.where(lane < LANES - NY, turned, edge) - here)

    def along_z(source, span, at):
        here = [gathered[p, source, span].astype(jnp.float32) for p in range(depth)]
        here.append(above[source, span].astype(jnp.float32))
        for p in range(depth):
            put(2, p, at, here[p + 1] - here[p])

    step_rows = 256

    def weigh(d, total):
        def one(i, total):
            at = pl.ds(pl.multiple_of(i * step_rows, step_rows), step_rows)
            mixed = jnp.dot(weight[at, :], diffs[d], preferred_element_type=jnp.float32)
            product = mixed * diffs[d, at, :].astype(jnp.float32)
            return total + jnp.sum(product.reshape(-1, 8, depth * LANES), axis=0)

        return lax.fori_loop(0, count // step_rows, one, total)

    total = jnp.zeros((8, depth * LANES), jnp.float32)
    each_block(along_y)
    weight_copy.wait()
    total = weigh(1, total)

    @pl.when(odd)
    def _():
        each_block(along_x_odd)

    @pl.when(jnp.logical_not(odd))
    def _():
        def arrive(chunk, carry):
            partner_copy(chunk).wait_recv()
            return carry

        lax.fori_loop(0, CHUNKS, arrive, 0)
        each_block(along_x_even)

    total = weigh(0, total)

    @pl.when(has_high)
    def _():
        def arrive(chunk, carry):
            above_copy(chunk).wait_recv()
            return carry

        lax.fori_loop(0, CHUNKS, arrive, 0)

    each_block(along_z)
    total = weigh(2, total)
    summed = jnp.sum(total, axis=0, keepdims=True) * (1.0 / count)
    for p in range(depth):
        grad[p : p + 1, :] = summed[:, p * LANES : (p + 1) * LANES]

    for present, side in sends:

        @pl.when(present)
        def _(side=side):
            sigma_copy(side).wait_send()

    def drain(chunk, carry):
        for present, side in sends:

            @pl.when(present)
            def _(side=side):
                halo_copy(side, chunk).wait_send()

        for r in range(1, groups):
            main_copy(r, chunk).wait_send()

            @pl.when(takes_side(lax.rem(j + r, groups)))
            def _(r=r):
                side_copy(r, chunk).wait_send()

        @pl.when(has_low)
        def _():
            above_copy(chunk).wait_send()

        @pl.when(odd)
        def _():
            partner_copy(chunk).wait_send()

        return carry

    lax.fori_loop(0, CHUNKS, drain, 0)


def body(conductivity, prev_fields, electrodes, data_weight):
    local, depth, plane = prev_fields.shape
    groups = lax.axis_size("src")
    count = groups * local
    prev = jnp.transpose(prev_fields, (1, 0, 2))
    vmem = pl.BlockSpec(memory_space=pltpu.VMEM)
    dma = pltpu.SemaphoreType.DMA
    bf16 = jnp.bfloat16
    planes, gradient = pl.pallas_call(
        kernel,
        out_shape=(
            jax.ShapeDtypeStruct((depth, local, plane), bf16),
            jax.ShapeDtypeStruct((depth, LANES), jnp.float32),
        ),
        in_specs=[vmem, vmem, vmem, pl.BlockSpec(memory_space=pl.ANY)],
        out_specs=(vmem, vmem),
        scratch_shapes=[
            pltpu.VMEM((2, 2, local, plane), bf16),
            pltpu.VMEM((2, 2, plane), jnp.float32),
            pltpu.VMEM((depth + 2, 8, plane), jnp.float32),
            pltpu.VMEM((depth + 2, GROUP, plane), jnp.float32),
            pltpu.VMEM((groups, local, LANES), bf16),
            pltpu.VMEM((depth, groups, local, LANES), bf16),
            pltpu.VMEM((depth, groups, local, LANES), bf16),
            pltpu.VMEM((groups, local, LANES), bf16),
            pltpu.VMEM((groups, local, LANES), bf16),
            pltpu.VMEM((count, count), bf16),
            pltpu.VMEM((3, count, depth * LANES), bf16),
            dma((2, CHUNKS)),
            dma((2, CHUNKS)),
            dma((2,)),
            dma((2,)),
            dma((groups - 1, CHUNKS)),
            dma((groups - 1, CHUNKS)),
            dma((groups - 1, CHUNKS)),
            dma((groups - 1, CHUNKS)),
            dma((CHUNKS,)),
            dma((CHUNKS,)),
            dma((CHUNKS,)),
            dma((CHUNKS,)),
            dma(()),
        ],
        compiler_params=pltpu.CompilerParams(
            collective_id=0, has_side_effects=True, vmem_limit_bytes=48 * 1024 * 1024
        ),
        name="step",
    )(conductivity, prev, electrodes, data_weight)
    return jnp.transpose(planes, (1, 0, 2)), gradient


def solution(mesh):
    placed = (P("cells", None), P("src", "cells", None), P("src", None), P())
    return jax.shard_map(
        body,
        mesh=mesh,
        in_specs=placed,
        out_specs=(P("src", "cells", None), P("cells", "src")),
        check_vma=False,
    )
```

```python
import jax
import jax.numpy as jnp
from jax import lax
from jax.experimental import pallas as pl
from jax.experimental.pallas import tpu as pltpu
from jax.sharding import PartitionSpec as P

NY = 32
LANES = 128
CHUNKS = 4
GROUP = 16
relaxation = 2.0 / 3.0
current = 4.0
ORDER = (1, 2, 3, 4, 5, 6, 7)
MESH = pl.DeviceIdType.MESH


def kernel(
    cond, prev, pairs, weight, pot, grad,
    halo, sigma_halo, coef, first, packed, gathered, partner, above, beside, electrodes, mixing,
    diffs,
    halo_send, halo_recv, sigma_send, sigma_recv, base_send, base_recv, main_send, main_recv,
    side_send, side_recv, above_send, above_recv, partner_send, partner_recv,
):
    slabs, groups = lax.axis_size("cells"), lax.axis_size("src")
    depth, local, plane = prev.shape
    tiles = plane // LANES
    rows = local // CHUNKS
    count = groups * local
    k, j = lax.axis_index("cells"), lax.axis_index("src")
    odd = lax.rem(j, 2) == 1
    has_low, has_high = k > 0, k < slabs - 1
    sided = jnp.logical_and(odd, j < groups - 1)

    barrier = pltpu.get_barrier_semaphore()

    @pl.when(has_low)
    def _():
        pl.semaphore_signal(barrier, inc=1, device_id=(k - 1, j), device_id_type=MESH)

    @pl.when(has_high)
    def _():
        pl.semaphore_signal(barrier, inc=1, device_id=(k + 1, j), device_id_type=MESH)

    for r in range(1, groups):
        pl.semaphore_signal(
            barrier, inc=1, device_id=(k, lax.rem(j + r, groups)), device_id_type=MESH
        )
    pl.semaphore_wait(
        barrier, groups - 1 + has_low.astype(jnp.int32) + has_high.astype(jnp.int32)
    )

    def sigma_copy(side):
        return pltpu.make_async_remote_copy(
            src_ref=cond.at[pl.ds(2 - 2 * side, 2)],
            dst_ref=sigma_halo.at[side],
            send_sem=sigma_send.at[side],
            recv_sem=sigma_recv.at[side],
            device_id=(k + 1 - 2 * side, j),
            device_id_type=MESH,
        )

    def halo_copy(side, chunk):
        span = pl.ds(pl.multiple_of(chunk * rows, rows), rows)
        return pltpu.make_async_remote_copy(
            src_ref=prev.at[pl.ds(2 - 2 * side, 2), span],
            dst_ref=halo.at[side, :, span],
            send_sem=halo_send.at[side, chunk],
            recv_sem=halo_recv.at[side, chunk],
            device_id=(k + 1 - 2 * side, j),
            device_id_type=MESH,
        )

    def base_copy(r, chunk):
        peer = lax.rem(j + r, groups)
        span = pl.ds(pl.multiple_of(chunk * rows, rows), rows)
        band = pl.ds(pl.multiple_of(peer * LANES, LANES), LANES)
        return pltpu.make_async_remote_copy(
            src_ref=pot.at[0, span, band],
            dst_ref=gathered.at[0, j, span],
            send_sem=base_send.at[r - 1, chunk],
            recv_sem=base_recv.at[r - 1, chunk],
            device_id=(k, peer),
            device_id_type=MESH,
        )

    def main_copy(r, chunk):
        peer = lax.rem(j + r, groups)
        span = pl.ds(pl.multiple_of(chunk * rows, rows), rows)
        band = pl.ds(pl.multiple_of(peer * LANES, LANES), LANES)
        return pltpu.make_async_remote_copy(
            src_ref=pot.at[pl.ds(1, depth - 1), span, band],
            dst_ref=gathered.at[pl.ds(1, depth - 1), j, span],
            send_sem=main_send.at[r - 1, chunk],
            recv_sem=main_recv.at[r - 1, chunk],
            device_id=(k, peer),
            device_id_type=MESH,
        )

    def side_copy(r, chunk):
        peer = lax.rem(j + r, groups)
        span = pl.ds(pl.multiple_of(chunk * rows, rows), rows)
        return pltpu.make_async_remote_copy(
            src_ref=packed.at[lax.rem(peer + 1, groups), span],
            dst_ref=beside.at[j, span],
            send_sem=side_send.at[r - 1, chunk],
            recv_sem=side_recv.at[r - 1, chunk],
            device_id=(k, peer),
            device_id_type=MESH,
        )

    def takes_side(peer):
        return jnp.logical_and(lax.rem(peer, 2) == 1, peer < groups - 1)

    def above_copy(chunk):
        span = pl.ds(pl.multiple_of(chunk * rows, rows), rows)
        return pltpu.make_async_remote_copy(
            src_ref=gathered.at[0, :, span],
            dst_ref=above.at[:, span],
            send_sem=above_send.at[chunk],
            recv_sem=above_recv.at[chunk],
            device_id=(k - 1, j),
            device_id_type=MESH,
        )

    def partner_copy(chunk):
        span = pl.ds(pl.multiple_of(chunk * rows, rows), rows)
        return pltpu.make_async_remote_copy(
            src_ref=gathered.at[:, :, span],
            dst_ref=partner.at[:, :, span],
            send_sem=partner_send.at[chunk],
            recv_sem=partner_recv.at[chunk],
            device_id=(k, lax.rem(j - 1 + groups, groups)),
            device_id_type=MESH,
        )

    sends = ((has_high, 0), (has_low, 1))
    for present, side in sends:

        @pl.when(present)
        def _(side=side):
            sigma_copy(side).start()

    for chunk in range(CHUNKS):
        for present, side in sends:

            @pl.when(present)
            def _(side=side, chunk=chunk):
                halo_copy(side, chunk).start()

    wide = jnp.concatenate([pairs[...], jnp.zeros((6, local), jnp.int32)], axis=0)
    electrodes[...] = jnp.transpose(wide)
    quarter = lax.broadcasted_iota(jnp.int32, (rows, LANES), 1) // rows

    def reorder(source, carry):
        for chunk in range(CHUNKS):
            at = pl.multiple_of(source * local + chunk * rows, rows)
            turned = []
            for other in range(groups):
                block = weight[pl.ds(at, rows), other * LANES : (other + 1) * LANES]
                block = block.astype(jnp.float32)
                turned.append(
                    [block]
                    + [pltpu.roll(block, step * rows, 1) for step in range(1, CHUNKS)]
                )
            to = pl.ds(pl.multiple_of(chunk * groups * rows + source * rows, rows), rows)
            for part in range(CHUNKS):
                for half in range(groups // CHUNKS):
                    q = [turned[half * CHUNKS + i][(i - part) % CHUNKS] for i in range(CHUNKS)]
                    value = q[0]
                    for i in range(1, CHUNKS):
                        value = jnp.where(quarter == i, q[i], value)
                    tile = part * (groups // CHUNKS) + half
                    mixing[to, tile * LANES : (tile + 1) * LANES] = value.astype(mixing.dtype)
        return carry

    lax.fori_loop(0, groups, reorder, 0)
    for chunk in range(1, CHUNKS):
        at = slice(chunk * groups * rows, (chunk + 1) * groups * rows)
        for other in range(chunk):
            to = slice(other * groups * rows, (other + 1) * groups * rows)
            both = mixing[at, to].astype(jnp.float32) + jnp.transpose(
                mixing[to, at].astype(jnp.float32)
            )
            mixing[at, to] = both.astype(mixing.dtype)

    receives = ((has_low, 0), (has_high, 1))
    for present, side in receives:

        @pl.when(jnp.logical_not(present))
        def _(side=side):
            sigma_halo[side] = jnp.zeros(sigma_halo.shape[1:], sigma_halo.dtype)
            halo[side] = jnp.zeros(halo.shape[1:], halo.dtype)

        @pl.when(present)
        def _(side=side):
            sigma_copy(side).wait_recv()

    @pl.when(jnp.logical_not(has_high))
    def _():
        above[...] = jnp.zeros(above.shape, above.dtype)

    @pl.when(j == groups - 1)
    def _():
        beside[...] = jnp.zeros(beside.shape, beside.dtype)

    cell = lax.broadcasted_iota(jnp.int32, (1, plane), 1)
    column = lax.rem(cell, NY)
    own = cond[...]
    low, high = sigma_halo[0], sigma_halo[1]
    sigma = (
        [low[i : i + 1] for i in range(2)]
        + [own[i : i + 1] for i in range(depth)]
        + [high[i : i + 1] for i in range(2)]
    )
    for p in range(depth + 2):
        s, down, up = sigma[p + 1], sigma[p], sigma[p + 2]
        y_up = jnp.where(column != NY - 1, pltpu.roll(s, plane - 1, 1), 0.0)
        y_down = jnp.where(column != 0, pltpu.roll(s, 1, 1), 0.0)
        x_up = jnp.where(cell < plane - NY, pltpu.roll(s, plane - NY, 1), 0.0)
        x_down = jnp.where(cell >= NY, pltpu.roll(s, NY, 1), 0.0)
        faces = [0.5 * (s + o) for o in (up, down, y_up, y_down, x_up, x_down)]
        diagonal = faces[0] + faces[1] + faces[2] + faces[3] + faces[4] + faces[5]
        scale = relaxation / diagonal
        center = jnp.full((1, plane), 1.0 - relaxation, jnp.float32)
        if p == 0:
            scale = jnp.where(has_low, scale, 0.0)
            center = jnp.where(has_low, center, 0.0)
        if p == depth + 1:
            scale = jnp.where(has_high, scale, 0.0)
            center = jnp.where(has_high, center, 0.0)
        terms = [
            faces[0] * scale,
            faces[1] * scale,
            jnp.where(column != NY - 1, faces[2] * scale, 0.0),
            jnp.where(column != 0, faces[3] * scale, 0.0),
            jnp.where(cell < plane - NY, faces[4] * scale, 0.0),
            jnp.where(cell >= NY, faces[5] * scale, 0.0),
            center,
            current * scale,
        ]
        for i, term in enumerate(terms):
            coef[p, i : i + 1, :] = term

    lane = lax.broadcasted_iota(jnp.int32, (GROUP, LANES), 1)
    first_cell = k * (depth * plane)

    def sweep(value, p, pair, store):
        low_cell = first_cell + (p - 1) * plane
        plus, minus = pair[0] - low_cell, pair[1] - low_cell
        mids = [value(p, v) for v in range(tiles)]
        ups = [pltpu.roll(m, LANES - NY, 1) for m in mids]
        downs = [pltpu.roll(m, NY, 1) for m in mids]
        for v in range(tiles):
            c = [coef[p, i : i + 1, v * LANES : (v + 1) * LANES] for i in range(8)]
            x_up = jnp.where(lane < LANES - NY, ups[v], ups[v + 1]) if v < tiles - 1 else ups[v]
            x_down = jnp.where(lane >= NY, downs[v], downs[v - 1]) if v > 0 else downs[v]
            total = c[6] * mids[v] + c[0] * value(p + 1, v) + c[1] * value(p - 1, v)
            total = total + c[2] * pltpu.roll(mids[v], LANES - 1, 1)
            total = total + c[3] * pltpu.roll(mids[v], 1, 1)
            total = total + c[4] * x_up + c[5] * x_down
            here = lane + v * LANES
            gain = jnp.broadcast_to(c[7], (GROUP, LANES))
            total = total + jnp.where(here == plus, gain, jnp.where(here == minus, -gain, 0.0))
            store(v, total)

    def relax_group(g):
        span = pl.ds(pl.multiple_of(g * GROUP, GROUP), GROUP)
        pair = electrodes[span, :]
        pair = [
            jnp.broadcast_to(pair[:, 0:1], (GROUP, LANES)),
            jnp.broadcast_to(pair[:, 1:2], (GROUP, LANES)),
        ]

        def start(q, v):
            at = slice(v * LANES, (v + 1) * LANES)
            if q < 1:
                block = halo[0, q + 1, span, at]
            elif q <= depth:
                block = prev[q - 1, span, at]
            else:
                block = halo[1, q - depth - 1, span, at]
            return block.astype(jnp.float32)

        for p in range(depth + 2):

            def keep(v, total, p=p):
                first[p, :, v * LANES : (v + 1) * LANES] = total

            sweep(start, p, pair, keep)

        heads = [[None] * depth for _ in range(tiles)]

        def middle(q, v):
            return first[q, :, v * LANES : (v + 1) * LANES]

        for p in range(1, depth + 1):

            def keep(v, total, p=p):
                pot[p - 1, span, v * LANES : (v + 1) * LANES] = total.astype(pot.dtype)
                if v % 2 == 0:
                    turned = total if p == 1 else pltpu.roll(total, (p - 1) * NY, 1)
                    if p == 1:
                        heads[v] = turned
                    else:
                        heads[v] = jnp.where(lane < (p - 1) * NY, heads[v], turned)

            sweep(middle, p, pair, keep)
        for v in range(0, tiles, 2):
            packed[v, span] = heads[v].astype(packed.dtype)

    per_chunk = rows // GROUP

    def relax_chunk(chunk, carry):
        for present, side in receives:

            @pl.when(present)
            def _(side=side):
                halo_copy(side, chunk).wait_recv()

        def one(g, carry):
            relax_group(chunk * per_chunk + g)
            return carry

        lax.fori_loop(0, per_chunk, one, 0)
        span = pl.ds(pl.multiple_of(chunk * rows, rows), rows)
        band = pl.ds(pl.multiple_of(j * LANES, LANES), LANES)
        for p in range(depth):
            gathered[p, j, span] = pot[p, span, band]

        @pl.when(sided)
        def _():
            beside[j, span] = packed[lax.rem(j + 1, groups), span]

        for r in ORDER:
            base_copy(r, chunk).start()

        send_rest(chunk)
        return carry

    def send_rest(chunk):
        for r in ORDER:
            main_copy(r, chunk).start()

            @pl.when(takes_side(lax.rem(j + r, groups)))
            def _(r=r):
                side_copy(r, chunk).start()

    lax.fori_loop(0, CHUNKS, relax_chunk, 0)

    def raise_base(chunk):
        for r in range(1, groups):
            base_copy(r, chunk).wait_recv()

        @pl.when(has_low)
        def _():
            above_copy(chunk).start()


    early = (2 * depth - 1) * LANES
    width = 3 * depth * LANES
    span_rows = groups * rows
    lane = lax.broadcasted_iota(jnp.int32, (rows, LANES), 1)
    inner = lax.rem(lane, NY) != NY - 1
    within = lane < LANES - NY

    def each_source(chunk, step):
        span = pl.ds(pl.multiple_of(chunk * rows, rows), rows)

        def one(source, carry):
            at = pl.ds(pl.multiple_of(chunk * span_rows + source * rows, rows), rows)
            step(source, span, at)
            return carry

        lax.fori_loop(0, groups, one, 0)

    def put(at, column, value):
        diffs[at, column * LANES : (column + 1) * LANES] = value.astype(diffs.dtype)

    def along_yz(source, span, at):
        here = [gathered[p, source, span].astype(jnp.float32) for p in range(depth)]
        for p in range(depth):
            put(at, p, jnp.where(inner, pltpu.roll(here[p], LANES - 1, 1), 0.0) - here[p])
        for p in range(depth - 1):
            put(at, depth + p, here[p + 1] - here[p])

    def along_x(source, span, at, edges):
        for p in range(depth):
            here = gathered[p, source, span].astype(jnp.float32)
            turned = pltpu.roll(here, LANES - NY, 1)
            put(at, 2 * depth - 1 + p, jnp.where(within, turned, edges(p)) - here)
        top = above[source, span].astype(jnp.float32)
        put(at, 3 * depth - 1, top - gathered[depth - 1, source, span].astype(jnp.float32))

    def along_x_odd(source, span, at):
        tail = beside[source, span].astype(jnp.float32)

        def edges(p):
            shift = (LANES - NY - NY * p) % LANES
            return pltpu.roll(tail, shift, 1) if shift else tail

        along_x(source, span, at, edges)

    def along_x_even(source, span, at):
        def edges(p):
            return pltpu.roll(partner[p, source, span].astype(jnp.float32), LANES - NY, 1)

        along_x(source, span, at, edges)

    def take_rest(chunk):
        for r in range(1, groups):
            main_copy(r, chunk).wait_recv()

            @pl.when(sided)
            def _(r=r):
                side_copy(r, chunk).wait_recv()

        @pl.when(odd)
        def _():
            partner_copy(chunk).start()

        each_source(chunk, along_yz)

    def take_edges(chunk):
        @pl.when(has_high)
        def _():
            above_copy(chunk).wait_recv()

        @pl.when(odd)
        def _():
            each_source(chunk, along_x_odd)

        @pl.when(jnp.logical_not(odd))
        def _():
            partner_copy(chunk).wait_recv()
            each_source(chunk, along_x_even)

    def weigh(chunk, low, high):
        at = slice(chunk * span_rows, (chunk + 1) * span_rows)
        reach = slice(0, (chunk + 1) * span_rows)
        value = jnp.dot(
            mixing[at, reach], diffs[reach, low:high], preferred_element_type=jnp.float32
        )
        value = value * diffs[at, low:high].astype(jnp.float32)
        return jnp.sum(value.reshape(-1, 8, high - low), axis=0)

    inside = jnp.zeros((8, early), jnp.float32)
    outside = jnp.zeros((8, width - early), jnp.float32)
    for chunk in range(CHUNKS - 1):
        raise_base(chunk)
        take_rest(chunk)
        inside = inside + weigh(chunk, 0, early)
    raise_base(CHUNKS - 1)
    for chunk in range(CHUNKS - 2):
        take_edges(chunk)
        outside = outside + weigh(chunk, early, width)
    take_rest(CHUNKS - 1)
    inside = inside + weigh(CHUNKS - 1, 0, early)
    for chunk in (CHUNKS - 2, CHUNKS - 1):
        take_edges(chunk)
        outside = outside + weigh(chunk, early, width)
    inside = jnp.sum(inside, axis=0, keepdims=True) * (1.0 / count)
    outside = jnp.sum(outside, axis=0, keepdims=True) * (1.0 / count)
    columns = [inside[:, i * LANES : (i + 1) * LANES] for i in range(2 * depth - 1)]
    columns += [outside[:, i * LANES : (i + 1) * LANES] for i in range(depth + 1)]
    for p in range(depth):
        last = columns[depth + p] if p < depth - 1 else columns[3 * depth - 1]
        grad[p : p + 1, :] = columns[p] + columns[2 * depth - 1 + p] + last

    for present, side in sends:

        @pl.when(present)
        def _(side=side):
            sigma_copy(side).wait_send()

    def drain(chunk, carry):
        for present, side in sends:

            @pl.when(present)
            def _(side=side):
                halo_copy(side, chunk).wait_send()

        for r in range(1, groups):
            base_copy(r, chunk).wait_send()
            main_copy(r, chunk).wait_send()

            @pl.when(takes_side(lax.rem(j + r, groups)))
            def _(r=r):
                side_copy(r, chunk).wait_send()

        @pl.when(has_low)
        def _():
            above_copy(chunk).wait_send()

        @pl.when(odd)
        def _():
            partner_copy(chunk).wait_send()

        return carry

    lax.fori_loop(0, CHUNKS, drain, 0)


def body(conductivity, prev_fields, electrodes, data_weight):
    local, depth, plane = prev_fields.shape
    groups = lax.axis_size("src")
    count = groups * local
    prev = jnp.transpose(prev_fields, (1, 0, 2))
    vmem = pl.BlockSpec(memory_space=pltpu.VMEM)
    dma = pltpu.SemaphoreType.DMA
    bf16 = jnp.bfloat16
    planes, gradient = pl.pallas_call(
        kernel,
        out_shape=(
            jax.ShapeDtypeStruct((depth, local, plane), bf16),
            jax.ShapeDtypeStruct((depth, LANES), jnp.float32),
        ),
        in_specs=[vmem] * 4,
        out_specs=(vmem, vmem),
        scratch_shapes=[
            pltpu.VMEM((2, 2, local, plane), bf16),
            pltpu.VMEM((2, 2, plane), jnp.float32),
            pltpu.VMEM((depth + 2, 8, plane), jnp.float32),
            pltpu.VMEM((depth + 2, GROUP, plane), jnp.float32),
            pltpu.VMEM((groups, local, LANES), bf16),
            pltpu.VMEM((depth, groups, local, LANES), bf16),
            pltpu.VMEM((depth, groups, local, LANES), bf16),
            pltpu.VMEM((groups, local, LANES), bf16),
            pltpu.VMEM((groups, local, LANES), bf16),
            pltpu.VMEM((local, 8), jnp.int32),
            pltpu.VMEM((count, count), bf16),
            pltpu.VMEM((count, 3 * depth * LANES), bf16),
            dma((2, CHUNKS)),
            dma((2, CHUNKS)),
            dma((2,)),
            dma((2,)),
            dma((groups - 1, CHUNKS)),
            dma((groups - 1, CHUNKS)),
            dma((groups - 1, CHUNKS)),
            dma((groups - 1, CHUNKS)),
            dma((groups - 1, CHUNKS)),
            dma((groups - 1, CHUNKS)),
            dma((CHUNKS,)),
            dma((CHUNKS,)),
            dma((CHUNKS,)),
            dma((CHUNKS,)),
        ],
        compiler_params=pltpu.CompilerParams(
            collective_id=0, has_side_effects=True, vmem_limit_bytes=48 * 1024 * 1024
        ),
        name="step",
    )(conductivity, prev, jnp.transpose(electrodes), data_weight)
    return jnp.transpose(planes, (1, 0, 2)), gradient


def solution(mesh):
    placed = (P("cells", None), P("src", "cells", None), P("src", None), P())
    return jax.shard_map(
        body,
        mesh=mesh,
        in_specs=placed,
        out_specs=(P("src", "cells", None), P("cells", "src")),
        check_vma=False,
    )
```

```python
import jax
import jax.numpy as jnp
from jax import lax
from jax.experimental import pallas as pl
from jax.experimental.pallas import tpu as pltpu
from jax.sharding import PartitionSpec as P

NY = 32
LANES = 128
CHUNKS = 4
GROUP = 16
relaxation = 2.0 / 3.0
current = 4.0
ORDER = (1, 2, 3, 4, 5, 6, 7)
MESH = pl.DeviceIdType.MESH


def kernel(
    cond_hbm, prev, pairs, weight, out, grad,
    halo, sigma_halo, coef, first, packed, gathered, partner, above, beside, electrodes, mixing,
    diffs, pot, cond, cond_sem,
    halo_send, halo_recv, sigma_send, sigma_recv, base_send, base_recv, main_send, main_recv,
    side_send, side_recv, above_send, above_recv, partner_send, partner_recv,
):
    slabs, groups = lax.axis_size("cells"), lax.axis_size("src")
    depth, local, plane = prev.shape
    tiles = plane // LANES
    rows = local // CHUNKS
    count = groups * local
    k, j = lax.axis_index("cells"), lax.axis_index("src")
    odd = lax.rem(j, 2) == 1
    has_low, has_high = k > 0, k < slabs - 1
    sided = jnp.logical_and(odd, j < groups - 1)

    cond_copy = pltpu.make_async_copy(cond_hbm, cond, cond_sem)
    cond_copy.start()

    barrier = pltpu.get_barrier_semaphore()

    @pl.when(has_low)
    def _():
        pl.semaphore_signal(barrier, inc=1, device_id=(k - 1, j), device_id_type=MESH)

    @pl.when(has_high)
    def _():
        pl.semaphore_signal(barrier, inc=1, device_id=(k + 1, j), device_id_type=MESH)

    for r in range(1, groups):
        pl.semaphore_signal(
            barrier, inc=1, device_id=(k, lax.rem(j + r, groups)), device_id_type=MESH
        )
    pl.semaphore_wait(
        barrier, groups - 1 + has_low.astype(jnp.int32) + has_high.astype(jnp.int32)
    )

    def sigma_copy(side):
        return pltpu.make_async_remote_copy(
            src_ref=cond_hbm.at[pl.ds(2 - 2 * side, 2)],
            dst_ref=sigma_halo.at[side],
            send_sem=sigma_send.at[side],
            recv_sem=sigma_recv.at[side],
            device_id=(k + 1 - 2 * side, j),
            device_id_type=MESH,
        )

    def halo_copy(side, chunk):
        span = pl.ds(pl.multiple_of(chunk * rows, rows), rows)
        return pltpu.make_async_remote_copy(
            src_ref=prev.at[pl.ds(2 - 2 * side, 2), span],
            dst_ref=halo.at[side, :, span],
            send_sem=halo_send.at[side, chunk],
            recv_sem=halo_recv.at[side, chunk],
            device_id=(k + 1 - 2 * side, j),
            device_id_type=MESH,
        )

    def base_copy(r, chunk):
        peer = lax.rem(j + r, groups)
        span = pl.ds(pl.multiple_of(chunk * rows, rows), rows)
        band = pl.ds(pl.multiple_of(peer * LANES, LANES), LANES)
        return pltpu.make_async_remote_copy(
            src_ref=pot.at[0, span, band],
            dst_ref=gathered.at[0, j, span],
            send_sem=base_send.at[r - 1, chunk],
            recv_sem=base_recv.at[r - 1, chunk],
            device_id=(k, peer),
            device_id_type=MESH,
        )

    def main_copy(r, chunk):
        peer = lax.rem(j + r, groups)
        span = pl.ds(pl.multiple_of(chunk * rows, rows), rows)
        band = pl.ds(pl.multiple_of(peer * LANES, LANES), LANES)
        return pltpu.make_async_remote_copy(
            src_ref=pot.at[pl.ds(1, depth - 1), span, band],
            dst_ref=gathered.at[pl.ds(1, depth - 1), j, span],
            send_sem=main_send.at[r - 1, chunk],
            recv_sem=main_recv.at[r - 1, chunk],
            device_id=(k, peer),
            device_id_type=MESH,
        )

    def side_copy(r, chunk):
        peer = lax.rem(j + r, groups)
        span = pl.ds(pl.multiple_of(chunk * rows, rows), rows)
        return pltpu.make_async_remote_copy(
            src_ref=packed.at[lax.rem(peer + 1, groups), span],
            dst_ref=beside.at[j, span],
            send_sem=side_send.at[r - 1, chunk],
            recv_sem=side_recv.at[r - 1, chunk],
            device_id=(k, peer),
            device_id_type=MESH,
        )

    def takes_side(peer):
        return jnp.logical_and(lax.rem(peer, 2) == 1, peer < groups - 1)

    def above_copy(chunk):
        span = pl.ds(pl.multiple_of(chunk * rows, rows), rows)
        return pltpu.make_async_remote_copy(
            src_ref=gathered.at[0, :, span],
            dst_ref=above.at[:, span],
            send_sem=above_send.at[chunk],
            recv_sem=above_recv.at[chunk],
            device_id=(k - 1, j),
            device_id_type=MESH,
        )

    def partner_copy(chunk):
        span = pl.ds(pl.multiple_of(chunk * rows, rows), rows)
        return pltpu.make_async_remote_copy(
            src_ref=gathered.at[:, :, span],
            dst_ref=partner.at[:, :, span],
            send_sem=partner_send.at[chunk],
            recv_sem=partner_recv.at[chunk],
            device_id=(k, lax.rem(j - 1 + groups, groups)),
            device_id_type=MESH,
        )

    sends = ((has_high, 0), (has_low, 1))
    for present, side in sends:

        @pl.when(present)
        def _(side=side):
            sigma_copy(side).start()

    for chunk in range(CHUNKS):
        for present, side in sends:

            @pl.when(present)
            def _(side=side, chunk=chunk):
                halo_copy(side, chunk).start()

    wide = jnp.concatenate([pairs[...], jnp.zeros((6, local), jnp.int32)], axis=0)
    electrodes[...] = jnp.transpose(wide)
    quarter = lax.broadcasted_iota(jnp.int32, (rows, LANES), 1) // rows

    def reorder(source, carry):
        for chunk in range(CHUNKS):
            at = pl.multiple_of(source * local + chunk * rows, rows)
            turned = []
            for other in range(groups):
                block = weight[pl.ds(at, rows), other * LANES : (other + 1) * LANES]
                block = block.astype(jnp.float32)
                turned.append(
                    [block]
                    + [pltpu.roll(block, step * rows, 1) for step in range(1, CHUNKS)]
                )
            to = pl.ds(pl.multiple_of(chunk * groups * rows + source * rows, rows), rows)
            for part in range(CHUNKS):
                for half in range(groups // CHUNKS):
                    q = [turned[half * CHUNKS + i][(i - part) % CHUNKS] for i in range(CHUNKS)]
                    value = q[0]
                    for i in range(1, CHUNKS):
                        value = jnp.where(quarter == i, q[i], value)
                    tile = part * (groups // CHUNKS) + half
                    mixing[to, tile * LANES : (tile + 1) * LANES] = value.astype(mixing.dtype)
        return carry

    lax.fori_loop(0, groups, reorder, 0)
    for chunk in range(1, CHUNKS):
        at = slice(chunk * groups * rows, (chunk + 1) * groups * rows)
        for other in range(chunk):
            to = slice(other * groups * rows, (other + 1) * groups * rows)
            both = mixing[at, to].astype(jnp.float32) + jnp.transpose(
                mixing[to, at].astype(jnp.float32)
            )
            mixing[at, to] = both.astype(mixing.dtype)

    receives = ((has_low, 0), (has_high, 1))
    for present, side in receives:

        @pl.when(jnp.logical_not(present))
        def _(side=side):
            sigma_halo[side] = jnp.zeros(sigma_halo.shape[1:], sigma_halo.dtype)
            halo[side] = jnp.zeros(halo.shape[1:], halo.dtype)

        @pl.when(present)
        def _(side=side):
            sigma_copy(side).wait_recv()

    @pl.when(jnp.logical_not(has_high))
    def _():
        above[...] = jnp.zeros(above.shape, above.dtype)

    @pl.when(j == groups - 1)
    def _():
        beside[...] = jnp.zeros(beside.shape, beside.dtype)

    cell = lax.broadcasted_iota(jnp.int32, (1, plane), 1)
    column = lax.rem(cell, NY)
    cond_copy.wait()
    own = cond[...]
    low, high = sigma_halo[0], sigma_halo[1]
    sigma = (
        [low[i : i + 1] for i in range(2)]
        + [own[i : i + 1] for i in range(depth)]
        + [high[i : i + 1] for i in range(2)]
    )
    for p in range(depth + 2):
        s, down, up = sigma[p + 1], sigma[p], sigma[p + 2]
        y_up = jnp.where(column != NY - 1, pltpu.roll(s, plane - 1, 1), 0.0)
        y_down = jnp.where(column != 0, pltpu.roll(s, 1, 1), 0.0)
        x_up = jnp.where(cell < plane - NY, pltpu.roll(s, plane - NY, 1), 0.0)
        x_down = jnp.where(cell >= NY, pltpu.roll(s, NY, 1), 0.0)
        faces = [0.5 * (s + o) for o in (up, down, y_up, y_down, x_up, x_down)]
        diagonal = faces[0] + faces[1] + faces[2] + faces[3] + faces[4] + faces[5]
        scale = relaxation / diagonal
        center = jnp.full((1, plane), 1.0 - relaxation, jnp.float32)
        if p == 0:
            scale = jnp.where(has_low, scale, 0.0)
            center = jnp.where(has_low, center, 0.0)
        if p == depth + 1:
            scale = jnp.where(has_high, scale, 0.0)
            center = jnp.where(has_high, center, 0.0)
        terms = [
            faces[0] * scale,
            faces[1] * scale,
            jnp.where(column != NY - 1, faces[2] * scale, 0.0),
            jnp.where(column != 0, faces[3] * scale, 0.0),
            jnp.where(cell < plane - NY, faces[4] * scale, 0.0),
            jnp.where(cell >= NY, faces[5] * scale, 0.0),
            center,
            current * scale,
        ]
        for i, term in enumerate(terms):
            coef[p, i : i + 1, :] = term

    lane = lax.broadcasted_iota(jnp.int32, (GROUP, LANES), 1)
    first_cell = k * (depth * plane)

    def sweep(value, p, pair, store):
        low_cell = first_cell + (p - 1) * plane
        plus, minus = pair[0] - low_cell, pair[1] - low_cell
        mids = [value(p, v) for v in range(tiles)]
        ups = [pltpu.roll(m, LANES - NY, 1) for m in mids]
        downs = [pltpu.roll(m, NY, 1) for m in mids]
        for v in range(tiles):
            c = [coef[p, i : i + 1, v * LANES : (v + 1) * LANES] for i in range(8)]
            x_up = jnp.where(lane < LANES - NY, ups[v], ups[v + 1]) if v < tiles - 1 else ups[v]
            x_down = jnp.where(lane >= NY, downs[v], downs[v - 1]) if v > 0 else downs[v]
            total = c[6] * mids[v] + c[0] * value(p + 1, v) + c[1] * value(p - 1, v)
            total = total + c[2] * pltpu.roll(mids[v], LANES - 1, 1)
            total = total + c[3] * pltpu.roll(mids[v], 1, 1)
            total = total + c[4] * x_up + c[5] * x_down
            here = lane + v * LANES
            gain = jnp.broadcast_to(c[7], (GROUP, LANES))
            total = total + jnp.where(here == plus, gain, jnp.where(here == minus, -gain, 0.0))
            store(v, total)

    def relax_group(g):
        span = pl.ds(pl.multiple_of(g * GROUP, GROUP), GROUP)
        pair = electrodes[span, :]
        pair = [
            jnp.broadcast_to(pair[:, 0:1], (GROUP, LANES)),
            jnp.broadcast_to(pair[:, 1:2], (GROUP, LANES)),
        ]

        def start(q, v):
            at = slice(v * LANES, (v + 1) * LANES)
            if q < 1:
                block = halo[0, q + 1, span, at]
            elif q <= depth:
                block = prev[q - 1, span, at]
            else:
                block = halo[1, q - depth - 1, span, at]
            return block.astype(jnp.float32)

        for p in range(depth + 2):

            def keep(v, total, p=p):
                first[p, :, v * LANES : (v + 1) * LANES] = total

            sweep(start, p, pair, keep)

        heads = [[None] * depth for _ in range(tiles)]

        def middle(q, v):
            return first[q, :, v * LANES : (v + 1) * LANES]

        for p in range(1, depth + 1):

            def keep(v, total, p=p):
                pot[p - 1, span, v * LANES : (v + 1) * LANES] = total.astype(pot.dtype)
                if v % 2 == 0:
                    turned = total if p == 1 else pltpu.roll(total, (p - 1) * NY, 1)
                    if p == 1:
                        heads[v] = turned
                    else:
                        heads[v] = jnp.where(lane < (p - 1) * NY, heads[v], turned)

            sweep(middle, p, pair, keep)
        for v in range(0, tiles, 2):
            packed[v, span] = heads[v].astype(packed.dtype)

    per_chunk = rows // GROUP

    def relax_chunk(chunk, carry):
        for present, side in receives:

            @pl.when(present)
            def _(side=side):
                halo_copy(side, chunk).wait_recv()

        def one(g, carry):
            relax_group(chunk * per_chunk + g)
            return carry

        lax.fori_loop(0, per_chunk, one, 0)
        span = pl.ds(pl.multiple_of(chunk * rows, rows), rows)
        band = pl.ds(pl.multiple_of(j * LANES, LANES), LANES)
        for p in range(depth):
            gathered[p, j, span] = pot[p, span, band]

        @pl.when(sided)
        def _():
            beside[j, span] = packed[lax.rem(j + 1, groups), span]

        for r in ORDER:
            base_copy(r, chunk).start()

        send_rest(chunk)
        return carry

    def send_rest(chunk):
        for r in ORDER:
            main_copy(r, chunk).start()

            @pl.when(takes_side(lax.rem(j + r, groups)))
            def _(r=r):
                side_copy(r, chunk).start()

    lax.fori_loop(0, CHUNKS, relax_chunk, 0)

    def regroup(g, carry):
        span = pl.ds(pl.multiple_of(g * GROUP, GROUP), GROUP)
        for v in range(tiles):
            at = slice(v * LANES, (v + 1) * LANES)
            parts = [pot[p, span, at].astype(jnp.float32) for p in range(depth)]
            out[span, :, at] = jnp.stack(parts, axis=1).astype(out.dtype)
        return carry

    lax.fori_loop(0, local // GROUP, regroup, 0)

    def raise_base(chunk):
        for r in range(1, groups):
            base_copy(r, chunk).wait_recv()

        @pl.when(has_low)
        def _():
            above_copy(chunk).start()


    early = (2 * depth - 1) * LANES
    width = 3 * depth * LANES
    span_rows = groups * rows
    lane = lax.broadcasted_iota(jnp.int32, (rows, LANES), 1)
    inner = lax.rem(lane, NY) != NY - 1
    within = lane < LANES - NY

    def each_source(chunk, step):
        span = pl.ds(pl.multiple_of(chunk * rows, rows), rows)

        def one(source, carry):
            at = pl.ds(pl.multiple_of(chunk * span_rows + source * rows, rows), rows)
            step(source, span, at)
            return carry

        lax.fori_loop(0, groups, one, 0)

    def put(at, column, value):
        diffs[at, column * LANES : (column + 1) * LANES] = value.astype(diffs.dtype)

    def along_yz(source, span, at):
        here = [gathered[p, source, span].astype(jnp.float32) for p in range(depth)]
        for p in range(depth):
            put(at, p, jnp.where(inner, pltpu.roll(here[p], LANES - 1, 1), 0.0) - here[p])
        for p in range(depth - 1):
            put(at, depth + p, here[p + 1] - here[p])

    def along_x(source, span, at, edges):
        for p in range(depth):
            here = gathered[p, source, span].astype(jnp.float32)
            turned = pltpu.roll(here, LANES - NY, 1)
            put(at, 2 * depth - 1 + p, jnp.where(within, turned, edges(p)) - here)
        top = above[source, span].astype(jnp.float32)
        put(at, 3 * depth - 1, top - gathered[depth - 1, source, span].astype(jnp.float32))

    def along_x_odd(source, span, at):
        tail = beside[source, span].astype(jnp.float32)

        def edges(p):
            shift = (LANES - NY - NY * p) % LANES
            return pltpu.roll(tail, shift, 1) if shift else tail

        along_x(source, span, at, edges)

    def along_x_even(source, span, at):
        def edges(p):
            return pltpu.roll(partner[p, source, span].astype(jnp.float32), LANES - NY, 1)

        along_x(source, span, at, edges)

    def take_rest(chunk):
        for r in range(1, groups):
            main_copy(r, chunk).wait_recv()

            @pl.when(sided)
            def _(r=r):
                side_copy(r, chunk).wait_recv()

        @pl.when(odd)
        def _():
            partner_copy(chunk).start()

        each_source(chunk, along_yz)

    def take_edges(chunk):
        @pl.when(has_high)
        def _():
            above_copy(chunk).wait_recv()

        @pl.when(odd)
        def _():
            each_source(chunk, along_x_odd)

        @pl.when(jnp.logical_not(odd))
        def _():
            partner_copy(chunk).wait_recv()
            each_source(chunk, along_x_even)

    def weigh(chunk, low, high):
        at = slice(chunk * span_rows, (chunk + 1) * span_rows)
        reach = slice(0, (chunk + 1) * span_rows)
        value = jnp.dot(
            mixing[at, reach], diffs[reach, low:high], preferred_element_type=jnp.float32
        )
        value = value * diffs[at, low:high].astype(jnp.float32)
        return jnp.sum(value.reshape(-1, 8, high - low), axis=0)

    inside = jnp.zeros((8, early), jnp.float32)
    outside = jnp.zeros((8, width - early), jnp.float32)
    for chunk in range(CHUNKS - 1):
        raise_base(chunk)
        take_rest(chunk)
        inside = inside + weigh(chunk, 0, early)
    raise_base(CHUNKS - 1)
    for chunk in range(CHUNKS - 2):
        take_edges(chunk)
        outside = outside + weigh(chunk, early, width)
    take_rest(CHUNKS - 1)
    inside = inside + weigh(CHUNKS - 1, 0, early)
    for chunk in (CHUNKS - 2, CHUNKS - 1):
        take_edges(chunk)
        outside = outside + weigh(chunk, early, width)
    inside = jnp.sum(inside, axis=0, keepdims=True) * (1.0 / count)
    outside = jnp.sum(outside, axis=0, keepdims=True) * (1.0 / count)
    columns = [inside[:, i * LANES : (i + 1) * LANES] for i in range(2 * depth - 1)]
    columns += [outside[:, i * LANES : (i + 1) * LANES] for i in range(depth + 1)]
    for p in range(depth):
        last = columns[depth + p] if p < depth - 1 else columns[3 * depth - 1]
        grad[p : p + 1, :] = columns[p] + columns[2 * depth - 1 + p] + last

    for present, side in sends:

        @pl.when(present)
        def _(side=side):
            sigma_copy(side).wait_send()

    def drain(chunk, carry):
        for present, side in sends:

            @pl.when(present)
            def _(side=side):
                halo_copy(side, chunk).wait_send()

        for r in range(1, groups):
            base_copy(r, chunk).wait_send()
            main_copy(r, chunk).wait_send()

            @pl.when(takes_side(lax.rem(j + r, groups)))
            def _(r=r):
                side_copy(r, chunk).wait_send()

        @pl.when(has_low)
        def _():
            above_copy(chunk).wait_send()

        @pl.when(odd)
        def _():
            partner_copy(chunk).wait_send()

        return carry

    lax.fori_loop(0, CHUNKS, drain, 0)


def body(conductivity, prev_fields, electrodes, data_weight):
    local, depth, plane = prev_fields.shape
    groups = lax.axis_size("src")
    count = groups * local
    prev = jnp.transpose(prev_fields, (1, 0, 2))
    vmem = pl.BlockSpec(memory_space=pltpu.VMEM)
    dma = pltpu.SemaphoreType.DMA
    bf16 = jnp.bfloat16
    return pl.pallas_call(
        kernel,
        out_shape=(
            jax.ShapeDtypeStruct((local, depth, plane), bf16),
            jax.ShapeDtypeStruct((depth, LANES), jnp.float32),
        ),
        in_specs=[pl.BlockSpec(memory_space=pltpu.HBM), vmem, vmem, vmem],
        out_specs=(vmem, vmem),
        scratch_shapes=[
            pltpu.VMEM((2, 2, local, plane), bf16),
            pltpu.VMEM((2, 2, plane), jnp.float32),
            pltpu.VMEM((depth + 2, 8, plane), jnp.float32),
            pltpu.VMEM((depth + 2, GROUP, plane), jnp.float32),
            pltpu.VMEM((groups, local, LANES), bf16),
            pltpu.VMEM((depth, groups, local, LANES), bf16),
            pltpu.VMEM((depth, groups, local, LANES), bf16),
            pltpu.VMEM((groups, local, LANES), bf16),
            pltpu.VMEM((groups, local, LANES), bf16),
            pltpu.VMEM((local, 8), jnp.int32),
            pltpu.VMEM((count, count), bf16),
            pltpu.VMEM((count, 3 * depth * LANES), bf16),
            pltpu.VMEM((depth, local, plane), bf16),
            pltpu.VMEM((depth, plane), jnp.float32),
            dma(()),
            dma((2, CHUNKS)),
            dma((2, CHUNKS)),
            dma((2,)),
            dma((2,)),
            dma((groups - 1, CHUNKS)),
            dma((groups - 1, CHUNKS)),
            dma((groups - 1, CHUNKS)),
            dma((groups - 1, CHUNKS)),
            dma((groups - 1, CHUNKS)),
            dma((groups - 1, CHUNKS)),
            dma((CHUNKS,)),
            dma((CHUNKS,)),
            dma((CHUNKS,)),
            dma((CHUNKS,)),
        ],
        compiler_params=pltpu.CompilerParams(
            collective_id=0, has_side_effects=True, vmem_limit_bytes=48 * 1024 * 1024
        ),
        name="step",
    )(
        pltpu.with_memory_space_constraint(conductivity, pltpu.HBM),
        prev,
        jnp.transpose(electrodes),
        data_weight,
    )


def solution(mesh):
    placed = (P("cells", None), P("src", "cells", None), P("src", None), P())
    return jax.shard_map(
        body,
        mesh=mesh,
        in_specs=placed,
        out_specs=(P("src", "cells", None), P("cells", "src")),
        check_vma=False,
    )
```
